256 devices in a mesh: pb: 2 (over y), col: 32 (over z, core), row: 4 (over x).
Axes of the slice: x: 4, y: 2, z: 16, core: 2. Of those that a mesh axis runs over, the one named last changes fastest.
The devices are a block of a 4x16x16 slice.
Arguments:
- pair_density: bfloat16 [6144, 6144], P(('pb', 'col'), 'row'), parts along dimension 0, may hold values from -0.19921875 to 0.19921875
- band_pairs: int32 [2, 3072], replicated, may hold values from 0 to 255, as said below
- valence: float32 [256], replicated, may hold values from -12 to -2
- conduction: float32 [12], replicated, may hold values from 1 to 8
- wave_vectors: int32 [3, 12288], P(None, 'pb'), parts along dimension 1, may hold values from -6 to 6
- momentum: float32 [6], P('pb'), parts along dimension 0, may hold values from 0.3 to 0.7
- guess_scale: float32 [12288], P('pb'), parts along dimension 0, may hold values from 0.4 to 0.75
Outputs:
- epsilon: float32 [12288, 6144], P(('pb', 'row'), 'col'), parts along dimension 0
- inverse: float32 [12288, 6144], P(('pb', 'row'), 'col'), parts along dimension 0
The draws below stay inside these ranges and needn't reach their ends.
There are 2 independent parts, one for each index of `pb`. The reference program is written for one: setup_inputs(seed, part) draws one part's arguments, and reference() takes and returns one part's arrays. A program takes and returns all parts, laid end to end along the dimension named above; an argument that names none is the same for every part. Nothing has to cross between parts.
Inputs may be any that keep to these rules, and one draw needn't show every extreme that they name: `band_pairs`: column p names a valence band below 256 in row 0 and a conduction band below 12 in row 1; every such pair of bands appears in exactly one column.
All inputs are finite; a program needn't handle non-finite values.
Results may differ from the reference program's by a relative error of at most 0.0036.
The reference program's roundings to bfloat16 on the way (of `weighted`, `mixed_b` and `square_b`) count: a program that leaves them out, or rounds other values in their place, can miss the bound.
Values may be sent and summed in bfloat16 or wider, within the bound.
No kernel may reach another device: no remote copies, remote signals or barrier semaphores. Data moves between devices by JAX's collectives and lax.ppermute only.
A program may use at most 64 MiB of HBM per device.

```python
import math
import jax
import jax.numpy as jnp
from jax import lax

NG = 6144
NV = 256
NC = 12
PAIRS = 3072


def draw_band_pairs(key, part):
    shuffled = jax.random.permutation(jax.random.fold_in(key, 17), NV * NC).astype(jnp.int32)
    return jnp.stack([shuffled // NC, shuffled % NC]).astype(jnp.int32)


def place_ends(result, stream_key, low, high):
    longest = result.shape.index(max(result.shape))
    spots = []
    for shift in (0, 1):
        where = [jax.random.randint(jax.random.fold_in(stream_key, axis), (), 0, length) for axis, length in enumerate(result.shape)]
        where[longest] = (where[longest] + shift) % result.shape[longest]
        spots.append(tuple(where))
    return result.at[spots[0]].set(low).at[spots[1]].set(high)


def spiked(array, key, source, target, parts, factor):
    owner, partner = [(jnp.arange(array.shape[position]) // (array.shape[position] // parts)).reshape([-1 if axis == position else 1 for axis in range(array.ndim)]) for position in (source, target)]
    chosen = jax.random.permutation(key, parts)[partner]
    strong = (owner == chosen) | (owner == (partner + parts // 2) % parts)
    return jnp.where(strong, factor * array, array)


def levels(stream_key, extent, pieces, low, high):
    gain, own = 1.0, jax.random.fold_in(stream_key, 6)
    for position, shards_of in pieces:
        steps = jnp.exp(jax.random.uniform(jax.random.fold_in(own, position), (shards_of,), jnp.float32, low / len(pieces), high / len(pieces)))
        gain = gain * jnp.repeat(steps, extent[position] // shards_of).reshape([-1 if axis == position else 1 for axis in range(len(extent))])
    return gain


def noise_with(rng, dims, deviation, reach, pieces, heavy, kind=jnp.bfloat16):
    result = deviation * jax.random.normal(rng, dims, jnp.float32)
    if pieces:
        result = result * levels(rng, dims, pieces, -0.22, 0.18)
    return jnp.clip(spiked(result, jax.random.fold_in(rng, 3), *heavy), -reach, reach).astype(kind)


def setup_inputs(seed: int = 0, part: int = 0) -> dict:
    keys = jax.random.split(jax.random.key(seed), 8)
    own_keys = jax.random.split(jax.random.fold_in(keys[7], part), 8)
    pair_density = noise_with(own_keys[0], (PAIRS, NG), 0.033, 0.19921875, ((0, 32), (1, 4)), (0, 1, 32, 2.75))
    band_pairs = draw_band_pairs(jax.random.fold_in(keys[7], 71), part)
    valence = jnp.clip(jax.random.uniform(keys[2], (NV,), jnp.float32, -12.0, -2.0), -12.0, -2.0)
    conduction = jnp.clip(jax.random.uniform(keys[3], (NC,), jnp.float32, 1.0, 8.0), 1.0, 8.0)
    wave_vectors = place_ends(jax.random.randint(own_keys[4], (3, NG), -6, 7), jax.random.fold_in(own_keys[4], 1), -6, 6).astype(jnp.int32)
    momentum = jnp.clip(jax.random.uniform(own_keys[5], (3,), jnp.float32, 0.3, 0.7), 0.3, 0.7)
    guess_scale = jnp.clip(jax.random.uniform(own_keys[6], (NG,), jnp.float32, 0.4, 0.75), 0.4, 0.75)
    return dict(pair_density=pair_density, band_pairs=band_pairs, valence=valence, conduction=conduction, wave_vectors=wave_vectors, momentum=momentum, guess_scale=guess_scale)


def reference(pair_density, band_pairs, valence, conduction, wave_vectors, momentum, guess_scale):
    shifted = wave_vectors.astype(jnp.float32) + momentum[:, None]
    squared_norm = lax.optimization_barrier(jnp.sum(shifted * shifted, axis=0))
    sqrt_v = jnp.sqrt(4.0 * math.pi / squared_norm)
    valence_of = valence[band_pairs[0].astype(jnp.int32)]
    conduction_of = conduction[band_pairs[1].astype(jnp.int32)]
    weight = 4.0 / (valence_of - conduction_of)
    weighted = (weight[:, None] * pair_density.astype(jnp.float32)).astype(jnp.bfloat16)
    chi_zero = jnp.dot(weighted.T, pair_density, preferred_element_type=jnp.float32)
    identity = jnp.eye(chi_zero.shape[0], dtype=jnp.float32)
    epsilon = identity - sqrt_v[:, None] * chi_zero * sqrt_v[None, :]
    guess = guess_scale / jnp.diagonal(epsilon)
    mixed = epsilon * guess[None, :]
    mixed_b = mixed.astype(jnp.bfloat16)
    square = jnp.dot(mixed_b, mixed_b, preferred_element_type=jnp.float32)
    square_b = square.astype(jnp.bfloat16)
    cube = jnp.dot(mixed_b, square_b, preferred_element_type=jnp.float32)
    inverse = guess[:, None] * (4.0 * identity - 6.0 * mixed + 4.0 * square - cube)
    return (epsilon, inverse)
```

```python
import math

import jax
import jax.numpy as jnp
from jax import lax
from jax.sharding import PartitionSpec as P

PARTS = 2


def lookup(indices, table):
    levels = jnp.arange(table.shape[0], dtype=jnp.int32)
    picked = indices[:, None] == levels[None, :]
    return jnp.sum(jnp.where(picked, table[None, :], 0.0), axis=1)


def gathered_pairs(own):
    devices = lax.axis_size("col")
    chips = devices // 2
    column = lax.axis_index("col")
    up = [(c, (c + 2) % devices) for c in range(devices)]
    down = [(c, (c - 2) % devices) for c in range(devices)]
    sibling = [(c, c ^ 1) for c in range(devices)]
    pieces = jnp.split(own, PARTS, 0)
    rising, falling = list(pieces), list(pieces)
    blocks = [(piece, 0, part) for part, piece in enumerate(pieces)]
    last = chips // 2
    for step in range(1, last + 1):
        for part in range(PARTS):
            if step < last or part % 2 == 0:
                rising[part] = lax.ppermute(rising[part], "col", up)
                blocks.append((rising[part], -2 * step, part))
            if step < last or part % 2 == 1:
                falling[part] = lax.ppermute(falling[part], "col", down)
                blocks.append((falling[part], 2 * step, part))
    arrays, origins = [], []
    for piece, offset, part in blocks:
        arrays += [piece, lax.ppermute(piece, "col", sibling)]
        origins += [((column + offset) % devices) * PARTS + part, ((column ^ 1) + offset) % devices * PARTS + part]
    return arrays, origins


def summed_over_rows(partial):
    count = lax.axis_size("row")
    here = lax.axis_index("row")
    pieces = partial.reshape(count, partial.shape[0] // count, partial.shape[1])
    total = lax.dynamic_index_in_dim(pieces, here, 0, keepdims=False)
    received = []
    for shift in (1, 3, 2):
        sent = lax.dynamic_index_in_dim(pieces, (here + shift) % count, 0, keepdims=False).astype(jnp.bfloat16)
        received.append(lax.ppermute(sent, "row", [(r, (r + shift) % count) for r in range(count)]))
    for piece in received:
        total = total + piece.astype(jnp.float32)
    own = total.astype(jnp.bfloat16)
    return lax.all_gather(own, "row", axis=0, tiled=True)


def on_device(pair_density, band_pairs, valence, conduction, wave_vectors, momentum, guess_scale):
    column_index = lax.axis_index("col")
    row_index = lax.axis_index("row")
    row_height = pair_density.shape[1]
    whole_width = row_height * lax.axis_size("row")
    strip_width = whole_width // lax.axis_size("col")
    valence_of = lookup(band_pairs[0], valence)
    conduction_of = lookup(band_pairs[1], conduction)
    weight = 4.0 / (valence_of - conduction_of)
    shifted = wave_vectors.astype(jnp.float32) + momentum[:, None]
    sqrt_all = jnp.sqrt(4.0 * math.pi / jnp.sum(shifted * shifted, axis=0))
    row_first = row_index * row_height
    column_first = column_index * strip_width
    sqrt_rows = lax.dynamic_slice_in_dim(sqrt_all, row_first, row_height, 0)
    sqrt_cols = lax.dynamic_slice_in_dim(sqrt_all, column_first, strip_width, 0)
    scale_rows = lax.dynamic_slice_in_dim(guess_scale, row_first, row_height, 0)
    scale_cols = lax.dynamic_slice_in_dim(guess_scale, column_first, strip_width, 0)

    arrays, origins = gathered_pairs(pair_density)
    panel = jnp.concatenate(arrays, axis=0)
    pieces = weight.reshape(len(arrays), -1)
    chosen = jnp.stack(origins)[:, None] == jnp.arange(len(arrays), dtype=jnp.int32)[None, :]
    weight = jnp.sum(jnp.where(chosen[:, :, None], pieces[None], 0.0), axis=1).reshape(-1)

    owner = column_first // row_height
    own_slice = lax.dynamic_slice_in_dim(panel, column_first % row_height, strip_width, 1)
    candidates = lax.all_gather(own_slice, "row", axis=0, tiled=False)
    strip = lax.dynamic_index_in_dim(candidates, owner, 0, keepdims=False)
    weighted = (weight[:, None] * panel.astype(jnp.float32)).astype(jnp.bfloat16)
    weighted_strip = (weight[:, None] * strip.astype(jnp.float32)).astype(jnp.bfloat16)

    def spread(pairs):
        return lax.dot_general(weighted, pairs, (((0,), (0,)), ((), ())), preferred_element_type=jnp.float32)

    chi_block = spread(strip)
    chi_rows = jnp.sum(weighted.astype(jnp.float32) * panel.astype(jnp.float32), axis=0)
    chi_cols = jnp.sum(weighted_strip.astype(jnp.float32) * strip.astype(jnp.float32), axis=0)
    global_rows = row_first + jnp.arange(row_height, dtype=jnp.int32)
    global_cols = column_first + jnp.arange(strip_width, dtype=jnp.int32)
    identity = (global_rows[:, None] == global_cols[None, :]).astype(jnp.float32)
    epsilon = identity - sqrt_rows[:, None] * chi_block * sqrt_cols[None, :]
    guess_rows = scale_rows / (1.0 - sqrt_rows * chi_rows * sqrt_rows)
    guess_cols = scale_cols / (1.0 - sqrt_cols * chi_cols * sqrt_cols)
    mixed = epsilon * guess_cols[None, :]

    def applied(block):
        rounded = block.astype(jnp.bfloat16).astype(jnp.float32)
        scaled = guess_rows[:, None] * rounded
        operand = (sqrt_rows[:, None] * scaled).astype(jnp.bfloat16)
        partial = jnp.dot(panel, operand, preferred_element_type=jnp.float32)
        return scaled - sqrt_rows[:, None] * spread(summed_over_rows(partial))

    square = applied(mixed)
    cube = applied(square)
    inverse = guess_rows[:, None] * (4.0 * identity - 6.0 * mixed + 4.0 * square - cube)
    return (epsilon, inverse)


def solution(mesh):
    placed = (P(("pb", "col"), "row"), P(), P(), P(), P(None, "pb"), P("pb"), P("pb"))
    return jax.shard_map(
        on_device,
        mesh=mesh,
        in_specs=placed,
        out_specs=(P(("pb", "row"), "col"), P(("pb", "row"), "col")),
        check_vma=False,
    )
```

```python
import functools
import math

import jax
import jax.numpy as jnp
from jax import lax
from jax.experimental import pallas as pl
from jax.experimental.pallas import tpu as pltpu
from jax.sharding import PartitionSpec as P


SHIFTS = (1, 3, 2)
LANES = 128
VMEM = pl.BlockSpec(memory_space=pltpu.VMEM)
SMEM = pl.BlockSpec(memory_space=pltpu.SMEM)
F32, BF16 = jnp.float32, jnp.bfloat16
shape = jax.ShapeDtypeStruct


def call(body, out_shape, operands, scratch=(), limit=4, scalars=(), flops=10**6):
    return pl.pallas_call(
        body,
        out_shape=out_shape,
        in_specs=[SMEM if i in scalars else VMEM for i in range(len(operands))],
        out_specs=jax.tree.map(lambda _: VMEM, out_shape),
        scratch_shapes=list(scratch),
        compiler_params=pltpu.CompilerParams(vmem_limit_bytes=limit << 20),
        cost_estimate=pl.CostEstimate(flops=flops, bytes_accessed=10**6, transcendentals=0),
    )(*operands)


def position():
    devices, count = lax.axis_size("col"), lax.axis_size("row")
    return lax.axis_index("col"), lax.axis_index("row"), devices, count


def setup_body(valence, conduction, momentum, bands, waves, scale, weight, sqrt_rows, sqrt_cols, scale_rows, scale_cols):
    column, here, _, _ = position()
    height, width = sqrt_rows.shape[1], sqrt_cols.shape[0]
    upper, lower = bands[0], bands[1]
    start = jnp.zeros(upper.shape, F32)
    valence_of = lax.fori_loop(0, valence.shape[0], lambda i, x: jnp.where(upper == i, valence[i], x), start, unroll=8)
    conduction_of = lax.fori_loop(0, conduction.shape[0], lambda i, x: jnp.where(lower == i, conduction[i], x), start)
    weight[...] = 4.0 / (valence_of - conduction_of)

    def root(at, size):
        total = None
        for i in range(waves.shape[0]):
            moved = waves[i : i + 1, pl.ds(at, size)].astype(F32) + momentum[i]
            total = moved * moved if total is None else total + moved * moved
        return jnp.sqrt(4.0 * math.pi / total)

    def turned(pair):
        one = jnp.where(column % 2 == 0, pair[:, :width], pair[:, width:])
        return jnp.broadcast_to(one, (LANES, width)).T

    first = pl.multiple_of(here * height, LANES)
    sqrt_rows[...] = root(first, height)
    scale_rows[...] = scale[:, pl.ds(first, height)]
    first = pl.multiple_of(column // 2 * (2 * width), LANES)
    sqrt_cols[...] = turned(root(first, 2 * width))
    scale_cols[...] = turned(scale[:, pl.ds(first, 2 * width)])


def factors(parts, weight, column, devices, rows):
    lane = lax.broadcasted_iota(jnp.int32, weight.shape, 1)
    core = column % 2
    found = []
    for steps, origin, first, size, _ in parts:
        chip = column - core + (4 * core - 2) * steps
        mine = lane == (chip + (core if origin is None else origin) + devices) % devices
        found.append(jnp.sum(jnp.where(mine, weight[...], 0.0), axis=1, keepdims=True)[first : first + size])
    return jnp.broadcast_to(jnp.concatenate(found, axis=0), (rows, LANES))


def weigh(at, block, factor, previous, weighted, turned, diagonal):
    wide = block.astype(F32)
    scaled = (factor * wide).astype(BF16)
    weighted[:, at] = scaled
    diagonal[:, at] = previous[:, at] + jnp.sum(scaled.astype(F32) * wide, axis=0, keepdims=True)
    turned[at, :] = block.T


def prepare_body(parts, weight, previous, *refs):
    pieces, (raw, turned, weighted, row, diagonal) = refs[: len(parts)], refs[len(parts) :]
    column, _, devices, _ = position()
    factor = factors(parts, weight, column, devices, weighted.shape[0])
    row[...] = factor.T[:1]

    def step(i, carry):
        at = pl.ds(pl.multiple_of(i * LANES, LANES), LANES)
        block = jnp.concatenate([r[f : f + n, at] for r, (*_, n, f) in zip(pieces, parts)], axis=0)
        raw[:, at] = block
        weigh(at, block, factor, previous, weighted, turned, diagonal)
        return carry

    lax.fori_loop(0, weighted.shape[1] // LANES, step, 0)


def finish_body(parts, weight, previous, raw, beside, turned, weighted, row, diagonal, strip):
    column, _, devices, _ = position()
    factor = factors(parts, weight, column + 1 - 2 * (column % 2), devices, weighted.shape[0])
    row[...] = factor.T[:1]

    def step(i, carry):
        at = pl.ds(pl.multiple_of(i * LANES, LANES), LANES)
        weigh(at, raw[:, at], factor, previous, weighted, turned, diagonal)
        return carry

    lax.fori_loop(0, weighted.shape[1] // LANES, step, 0)
    height, rows = strip.shape[0], raw.shape[0]
    first = pl.multiple_of((column * height) % turned.shape[0], 16)
    strip[:, :rows] = beside[pl.ds(first, height), :]
    strip[:, rows:] = turned[pl.ds(first, height), :]


def join_body(own, beside, out):
    column, _, _, _ = position()
    rows, core = own.shape[0], column % 2

    @pl.when(core == 0)
    def _():
        out[:rows], out[rows:] = own[...], beside[...]

    @pl.when(core == 1)
    def _():
        out[:rows], out[rows:] = beside[...], own[...]


def half_body(block, out):
    column, _, _, _ = position()
    rows = out.shape[0]
    out[...] = block[pl.ds(pl.multiple_of(column % 2 * rows, 16), rows), :]


def gate_body(token, out):
    out[...] = token[...]


def send_products(operand, turned, sends):
    size, at = sends.shape[2], 0
    for block in turned:
        rows = block.shape[1]
        first = at % size
        product = jnp.dot(operand[...], block[...], preferred_element_type=F32)
        sends[at // size, :, first : first + rows] = product.astype(BF16)
        at += rows


def unit_at(block_shape, first, height):
    column, here, _, _ = position()
    rows = lax.broadcasted_iota(jnp.int32, block_shape, 1) + (here * height + first)
    return rows == lax.broadcasted_iota(jnp.int32, block_shape, 0) + column * block_shape[0]


def summed(operand, weighted, at):
    total, first = None, 0
    for block in weighted:
        rows = block.shape[0]
        given = operand[:, first : first + rows] if len(operand.shape) == 2 else (
            operand[first // operand.shape[2], :, first % operand.shape[2] : first % operand.shape[2] + rows]
        )
        product = jnp.dot(given, block[:, at], preferred_element_type=F32)
        total = product if total is None else total + product
        first += rows
    return total


CHUNK = 256


def chunks(width, body):
    def step(i, carry):
        body(i * CHUNK, pl.ds(pl.multiple_of(i * CHUNK, CHUNK), CHUNK))
        return carry

    lax.fori_loop(0, width // CHUNK, step, 0)


def start_body(n, sqrt_rows, sqrt_cols, scale_rows, scale_cols, diagonal, token, *refs):
    strips, rows, refs = refs[: 4 * n], refs[4 * n : 6 * n], refs[6 * n :]
    weighted, turned, refs = refs[: 2 * n], refs[2 * n : 4 * n], refs[4 * n :]
    epsilon, mixed, guess_rows, sends, chosen, operand, line = refs
    column, here, _, count = position()
    width, height = mixed.shape
    relative = (here + count - (column * width) // height) % count
    at = 0
    for i in range(n):
        size = strips[4 * i].shape[1]
        for j in range(4):

            @pl.when(relative == j)
            def _():
                chosen[:, at : at + size] = strips[4 * i + j][...]

        at += size
    at = 0
    for row in rows:
        line[:, at : at + row.shape[1]] = row[...]
        at += row.shape[1]

    def add(i, total):
        lanes = pl.ds(pl.multiple_of(i * LANES, LANES), LANES)
        wide = chosen[:, lanes].astype(F32)
        return total + (line[:, lanes] * wide).astype(BF16).astype(F32) * wide

    total = lax.fori_loop(0, chosen.shape[1] // LANES, add, jnp.zeros((width, LANES), F32))
    chi_cols = jnp.sum(total, axis=1, keepdims=True)
    s_cols = sqrt_cols[:, :1]
    g_cols = scale_cols[:, :1] / (1.0 - s_cols * chi_cols * s_cols)
    s_all = sqrt_rows[...]
    guess_rows[...] = scale_rows[...] / (1.0 - s_all * diagonal[...] * s_all)

    def part(first, at):
        s_rows, g_rows = sqrt_rows[:, at], guess_rows[:, at]
        block = jnp.where(unit_at((width, CHUNK), first, height), 1.0, 0.0) - s_cols * summed(chosen, weighted, at) * s_rows
        epsilon[:, at] = block
        found = block * g_cols
        mixed[:, at] = found
        operand[:, at] = (s_rows * (g_rows * found.astype(BF16).astype(F32))).astype(BF16)

    chunks(height, part)
    send_products(operand, turned, sends)


def combine_body(parts, out):
    total = parts[0].astype(F32)
    for i in range(1, parts.shape[0]):
        total += parts[i].astype(F32)
    total = total.astype(BF16)
    for i in range(parts.shape[0]):
        out[i] = total


def middle_body(n, sqrt_rows, guess_rows, mixed, *refs):
    filled, *refs = refs
    weighted, turned, refs = refs[:n], refs[n : 2 * n], refs[2 * n :]
    square, sends, operand = refs

    def part(first, at):
        s_rows, g_rows = sqrt_rows[:, at], guess_rows[:, at]
        value = g_rows * mixed[:, at].astype(BF16).astype(F32) - s_rows * summed(filled, weighted, at)
        square[:, at] = value
        operand[:, at] = (s_rows * (g_rows * value.astype(BF16).astype(F32))).astype(BF16)

    chunks(mixed.shape[1], part)
    send_products(operand, turned, sends)


def final_body(sqrt_rows, guess_rows, mixed, square, *refs):
    filled, weighted, inverse = refs[0], refs[1:-1], refs[-1]
    width, height = mixed.shape

    def part(first, at):
        s_rows, g_rows, s = sqrt_rows[:, at], guess_rows[:, at], square[:, at]
        cube = g_rows * s.astype(BF16).astype(F32) - s_rows * summed(filled, weighted, at)
        unit = jnp.where(unit_at((width, CHUNK), first, height), 4.0, 0.0)
        inverse[:, at] = g_rows * (unit - 6.0 * mixed[:, at] + 4.0 * s - cube)

    chunks(height, part)


def on_device(pair_density, band_pairs, valence, conduction, wave_vectors, momentum, guess_scale):
    devices, count = lax.axis_size("col"), lax.axis_size("row")
    own_pairs, height = pair_density.shape
    width = height * count // devices
    pairs = own_pairs * devices
    sibling = [(c, c ^ 1) for c in range(devices)]
    last = devices // 4

    def shifted(array, shift):
        return lax.ppermute(array, "row", [(r, (r + shift) % count) for r in range(count)])

    beside = lax.ppermute(pair_density, "col", sibling)
    ring = [call(join_body, shape((2 * own_pairs, height), BF16), [pair_density, beside])]
    onward = [(c, (c + 2 - 4 * (c % 2)) % devices) for c in range(devices)]
    token = jnp.zeros((8, LANES), F32)
    for step in range(1, last + 1):
        block = ring[-1]
        if step == last:
            block = call(half_body, shape((own_pairs, height), BF16), [block])
        ring.append(lax.ppermute(block, "col", onward))
        token = call(gate_body, shape(token.shape, F32), [token])

    bands = band_pairs.reshape(2, devices, own_pairs).transpose(0, 2, 1)
    weight, sqrt_rows, sqrt_cols, scale_rows, scale_cols = call(
        setup_body,
        (
            shape((own_pairs, devices), F32),
            shape((1, height), F32),
            shape((width, LANES), F32),
            shape((1, height), F32),
            shape((width, LANES), F32),
        ),
        [valence, conduction, momentum, bands, wave_vectors, guess_scale[None, :]],
        scalars=(0, 1, 2),
    )
    turned, weighted, rows, strips = [], [], [], []
    diagonal = jnp.zeros((1, height), F32)

    def group(parts, pieces):
        nonlocal diagonal
        size, row = sum(part[3] for part in parts), shape((1, height), F32)
        made = (shape((height, size), BF16), shape((size, height), BF16), shape((1, size), F32), row)
        raw, t, w, line, diagonal = call(
            functools.partial(prepare_body, parts), (shape((size, height), BF16), *made), [weight, diagonal, *pieces]
        )
        raw = lax.ppermute(raw, "col", sibling)
        turn, weigh, row, diagonal, strip = call(
            functools.partial(finish_body, parts), (*made, shape((width, 2 * size), BF16)), [weight, diagonal, raw, t]
        )
        above, below, far = (shifted(strip, shift) for shift in SHIFTS)
        strips.extend([strip, above, far, below])
        rows.extend([line, row])
        turned.extend([t, turn])
        weighted.extend([w, weigh])

    def whole(*steps):
        return tuple((step, core, 0, own_pairs, core * own_pairs) for step in steps for core in range(2))

    def pieces_of(*steps):
        return [ring[step] for step in steps for _ in range(2)]

    rest = 2 * own_pairs // 3
    for first in (1, 3, 5):
        group(whole(first, first + 1), pieces_of(first, first + 1))
    group(whole(last - 1) + ((0, None, 0, rest, 0),), pieces_of(last - 1) + [pair_density])
    group(((0, None, rest, own_pairs - rest, rest), (last, None, 0, own_pairs, 0)), [pair_density, ring[last]])

    n = len(strips) // 4

    size = pairs // count
    tall, flat = (width, size), (width, height)
    traded = shape((count, *tall), BF16)
    filled = pltpu.VMEM((width, pairs), BF16)
    operand = pltpu.VMEM(flat, BF16)

    def swapped(array):
        return lax.all_to_all(array, "row", split_axis=0, concat_axis=0, tiled=True)

    def exchange(sends):
        return swapped(call(combine_body, shape((count, *tall), BF16), [swapped(sends)]))

    epsilon, mixed, guess_rows, sends = call(
        functools.partial(start_body, n),
        (shape(flat, F32), shape(flat, F32), shape((1, height), F32), traded),
        [sqrt_rows, sqrt_cols, scale_rows, scale_cols, diagonal, token, *strips, *rows, *weighted, *turned],
        [filled, operand, pltpu.VMEM((1, pairs), F32)],
        limit=12,
    )
    pieces = exchange(sends)
    square, sends = call(
        functools.partial(middle_body, 2 * n),
        (shape(flat, F32), traded),
        [sqrt_rows, guess_rows, mixed, pieces, *weighted, *turned],
        [operand],
        limit=12,
    )
    pieces = exchange(sends)
    inverse = call(final_body, shape(flat, F32), [sqrt_rows, guess_rows, mixed, square, pieces, *weighted], limit=12)
    return (epsilon.T, inverse.T)


def solution(mesh):
    placed = (P(("pb", "col"), "row"), P(), P(), P(), P(None, "pb"), P("pb"), P("pb"))

    return jax.shard_map(
        on_device,
        mesh=mesh,
        in_specs=placed,
        out_specs=(P(("pb", "row"), "col"), P(("pb", "row"), "col")),
        check_vma=False,
    )
```

```python
import functools
import math

import jax
import jax.numpy as jnp
from jax import lax
from jax.experimental import pallas as pl
from jax.experimental.pallas import tpu as pltpu
from jax.sharding import PartitionSpec as P


LANES = 128
SHIFTS = (1, 3, 2)
VMEM = pl.BlockSpec(memory_space=pltpu.VMEM)
SMEM = pl.BlockSpec(memory_space=pltpu.SMEM)
F32, BF16 = jnp.float32, jnp.bfloat16
shape = jax.ShapeDtypeStruct


def call(body, out_shape, operands, scratch=(), limit=4, scalars=(), flops=10**6):
    return pl.pallas_call(
        body,
        out_shape=out_shape,
        in_specs=[SMEM if i in scalars else VMEM for i in range(len(operands))],
        out_specs=jax.tree.map(lambda _: VMEM, out_shape),
        scratch_shapes=list(scratch),
        compiler_params=pltpu.CompilerParams(vmem_limit_bytes=limit << 20),
        cost_estimate=pl.CostEstimate(flops=flops, bytes_accessed=10**6, transcendentals=0),
    )(*operands)


def position():
    devices, count = lax.axis_size("col"), lax.axis_size("row")
    return lax.axis_index("col"), lax.axis_index("row"), devices, count


def setup_body(valence, conduction, momentum, bands, waves, scale, weight, sqrt_rows, sqrt_cols, scale_rows, scale_cols):
    column, here, _, _ = position()
    height, width = sqrt_rows.shape[1], sqrt_cols.shape[0]
    upper, lower = bands[0], bands[1]
    start = jnp.zeros(upper.shape, F32)
    valence_of = lax.fori_loop(0, valence.shape[0], lambda i, x: jnp.where(upper == i, valence[i], x), start, unroll=8)
    conduction_of = lax.fori_loop(0, conduction.shape[0], lambda i, x: jnp.where(lower == i, conduction[i], x), start)
    weight[...] = 4.0 / (valence_of - conduction_of)

    def root(at, size):
        total = None
        for i in range(waves.shape[0]):
            moved = waves[i : i + 1, pl.ds(at, size)].astype(F32) + momentum[i]
            total = moved * moved if total is None else total + moved * moved
        return jnp.sqrt(4.0 * math.pi / total)

    def turned(pair):
        one = jnp.where(column % 2 == 0, pair[:, :width], pair[:, width:])
        return jnp.broadcast_to(one, (LANES, width)).T

    first = pl.multiple_of(here * height, LANES)
    sqrt_rows[...] = root(first, height)
    scale_rows[...] = scale[:, pl.ds(first, height)]
    first = pl.multiple_of(column // 2 * (2 * width), LANES)
    sqrt_cols[...] = turned(root(first, 2 * width))
    scale_cols[...] = turned(scale[:, pl.ds(first, 2 * width)])


def factors(parts, weight, core, devices, rows):
    lane = lax.broadcasted_iota(jnp.int32, weight.shape, 1)
    found = []
    for offset, first, size, _ in parts:
        mine = lane == (core + offset + devices) % devices
        found.append(jnp.sum(jnp.where(mine, weight[...], 0.0), axis=1, keepdims=True)[first : first + size])
    return jnp.broadcast_to(jnp.concatenate(found, axis=0), (rows, LANES))


def weigh(at, block, factor, previous, weighted, turned, diagonal):
    wide = block.astype(F32)
    scaled = (factor * wide).astype(BF16)
    weighted[:, at] = scaled
    diagonal[:, at] = previous[:, at] + jnp.sum(scaled.astype(F32) * wide, axis=0, keepdims=True)
    turned[at, :] = block.T


def prepare_body(parts, weight, previous, *refs):
    pieces, (raw, turned, weighted, row, diagonal) = refs[: len(parts)], refs[len(parts) :]
    column, _, devices, _ = position()
    factor = factors(parts, weight, column, devices, weighted.shape[0])
    row[...] = factor.T[:1]

    def step(i, carry):
        at = pl.ds(pl.multiple_of(i * LANES, LANES), LANES)
        block = jnp.concatenate([r[f : f + n, at] for r, (_, _, n, f) in zip(pieces, parts)], axis=0)
        raw[:, at] = block
        weigh(at, block, factor, previous, weighted, turned, diagonal)
        return carry

    lax.fori_loop(0, weighted.shape[1] // LANES, step, 0)


def finish_body(parts, weight, previous, raw, beside, *refs):
    *earlier, turned, weighted, row, diagonal, strip = refs
    column, _, devices, _ = position()
    factor = factors(parts, weight, column + 1 - 2 * (column % 2), devices, weighted.shape[0])
    row[...] = factor.T[:1]

    def step(i, carry):
        at = pl.ds(pl.multiple_of(i * LANES, LANES), LANES)
        weigh(at, raw[:, at], factor, previous, weighted, turned, diagonal)
        return carry

    lax.fori_loop(0, weighted.shape[1] // LANES, step, 0)
    height, at = strip.shape[0], 0
    first = pl.multiple_of((column * height) % turned.shape[0], 16)
    for ref in earlier:
        strip[:, : ref.shape[1]] = ref[...]
        at = ref.shape[1]
    for ref in (beside, turned):
        strip[:, at : at + ref.shape[1]] = ref[pl.ds(first, height), :]
        at += ref.shape[1]


def gate_body(token, out):
    out[...] = token[...]


def send_products(operand, turned, sends):
    size, at = sends.shape[2], 0
    for block in turned:
        rows = block.shape[1]
        first = at % size
        product = jnp.dot(operand[...], block[...], preferred_element_type=F32)
        sends[at // size, :, first : first + rows] = product.astype(BF16)
        at += rows


def unit_at(block_shape, first, height):
    column, here, _, _ = position()
    rows = lax.broadcasted_iota(jnp.int32, block_shape, 1) + (here * height + first)
    return rows == lax.broadcasted_iota(jnp.int32, block_shape, 0) + column * block_shape[0]


def summed(operand, weighted, at):
    total, first = None, 0
    for block in weighted:
        rows = block.shape[0]
        product = jnp.dot(operand[:, first : first + rows], block[:, at], preferred_element_type=F32)
        total = product if total is None else total + product
        first += rows
    return total


CHUNK = 512


def chunks(width, body):
    def step(i, carry):
        body(i * CHUNK, pl.ds(pl.multiple_of(i * CHUNK, CHUNK), CHUNK))
        return carry

    lax.fori_loop(0, width // CHUNK, step, 0)


def start_body(n, sent, sqrt_rows, sqrt_cols, scale_rows, scale_cols, diagonal, token, *refs):
    strips, refs = refs[: 4 * sent], refs[4 * sent :]
    rows, refs = refs[: 2 * n], refs[2 * n :]
    weighted, turned, refs = refs[: 2 * n], refs[2 * n : 4 * n], refs[4 * n :]
    epsilon, mixed, guess_rows, sends, chosen, operand, line = refs
    column, here, _, count = position()
    width, height = mixed.shape
    relative = (here + count - (column * width) // height) % count
    at = 0
    for i in range(sent):
        size = strips[4 * i].shape[1]
        for j in range(4):

            @pl.when(relative == j)
            def _():
                chosen[:, at : at + size] = strips[4 * i + j][...]

        at += size
    at = 0
    for row in rows:
        line[:, at : at + row.shape[1]] = row[...]
        at += row.shape[1]

    def add(i, total):
        lanes = pl.ds(pl.multiple_of(i * LANES, LANES), LANES)
        wide = chosen[:, lanes].astype(F32)
        return total + (line[:, lanes] * wide).astype(BF16).astype(F32) * wide

    total = lax.fori_loop(0, chosen.shape[1] // LANES, add, jnp.zeros((width, LANES), F32))
    chi_cols = jnp.sum(total, axis=1, keepdims=True)
    s_cols = sqrt_cols[:, :1]
    g_cols = scale_cols[:, :1] / (1.0 - s_cols * chi_cols * s_cols)
    s_all = sqrt_rows[...]
    guess_rows[...] = scale_rows[...] / (1.0 - s_all * diagonal[...] * s_all)

    def part(first, at):
        s_rows, g_rows = sqrt_rows[:, at], guess_rows[:, at]
        block = jnp.where(unit_at((width, CHUNK), first, height), 1.0, 0.0) - s_cols * summed(chosen, weighted, at) * s_rows
        epsilon[:, at] = block
        found = block * g_cols
        mixed[:, at] = found
        operand[:, at] = (s_rows * (g_rows * found.astype(BF16).astype(F32))).astype(BF16)

    chunks(height, part)
    send_products(operand, turned, sends)


def combine_body(parts, out):
    total = parts[0].astype(F32)
    for i in range(1, parts.shape[0]):
        total += parts[i].astype(F32)
    out[...] = total.astype(BF16)


def fill(pieces, filled):
    _, here, _, count = position()
    size = pieces[0].shape[1]
    for shift, piece in zip((0, *SHIFTS), pieces):
        at = (here + count - shift) % count * size
        filled[:, pl.ds(pl.multiple_of(at, LANES), size)] = piece[...]


def middle_body(n, sqrt_rows, guess_rows, mixed, *refs):
    pieces, refs = refs[:4], refs[4:]
    weighted, turned, refs = refs[:n], refs[n : 2 * n], refs[2 * n :]
    square, sends, operand, filled = refs
    fill(pieces, filled)

    def part(first, at):
        s_rows, g_rows = sqrt_rows[:, at], guess_rows[:, at]
        value = g_rows * mixed[:, at].astype(BF16).astype(F32) - s_rows * summed(filled, weighted, at)
        square[:, at] = value
        operand[:, at] = (s_rows * (g_rows * value.astype(BF16).astype(F32))).astype(BF16)

    chunks(mixed.shape[1], part)
    send_products(operand, turned, sends)


def final_body(n, sqrt_rows, guess_rows, mixed, square, *refs):
    pieces, weighted, (inverse, filled) = refs[:4], refs[4 : 4 + n], refs[4 + n :]
    fill(pieces, filled)
    width, height = mixed.shape

    def part(first, at):
        s_rows, g_rows, s = sqrt_rows[:, at], guess_rows[:, at], square[:, at]
        cube = g_rows * s.astype(BF16).astype(F32) - s_rows * summed(filled, weighted, at)
        unit = jnp.where(unit_at((width, CHUNK), first, height), 4.0, 0.0)
        inverse[:, at] = g_rows * (unit - 6.0 * mixed[:, at] + 4.0 * s - cube)

    chunks(height, part)


def on_device(pair_density, band_pairs, valence, conduction, wave_vectors, momentum, guess_scale):
    devices, count = lax.axis_size("col"), lax.axis_size("row")
    own_pairs, height = pair_density.shape
    width = height * count // devices
    pairs = own_pairs * devices
    up = [(c, (c + 2) % devices) for c in range(devices)]
    down = [(c, (c - 2) % devices) for c in range(devices)]
    sibling = [(c, c ^ 1) for c in range(devices)]
    half, last = own_pairs // 2, devices // 4

    owner_of = [c * width // height for c in range(devices)]
    from_owner = [[(c * count + o, c * count + (o + s) % count) for c, o in enumerate(owner_of)] for s in (1, 2, 3)]

    onward = [(c * count + (o + 3) % count, c * count + (o + 2) % count) for c, o in enumerate(owner_of)]
    rising, falling = [pair_density], [pair_density]
    token = jnp.zeros((8, LANES), F32)
    for step in range(1, last + 1):
        r, f = rising[-1], falling[-1]
        if step == last:
            r, f = r[:half], f[half:]
        rising.append(lax.ppermute(r, "col", up))
        falling.append(lax.ppermute(f, "col", down))
        token = call(gate_body, shape(token.shape, F32), [token])

    bands = band_pairs.reshape(2, devices, own_pairs).transpose(0, 2, 1)
    weight, sqrt_rows, sqrt_cols, scale_rows, scale_cols = call(
        setup_body,
        (
            shape((own_pairs, devices), F32),
            shape((1, height), F32),
            shape((width, LANES), F32),
            shape((1, height), F32),
            shape((width, LANES), F32),
        ),
        [valence, conduction, momentum, bands, wave_vectors, guess_scale[None, :]],
        scalars=(0, 1, 2),
    )
    turned, weighted, rows, strips = [], [], [], []
    diagonal = jnp.zeros((1, height), F32)

    held = []

    def group(parts, pieces, send):
        nonlocal diagonal
        label = str(len(rows) // 2)
        size, row = sum(n for _, _, n, _ in parts), shape((1, height), F32)
        made = (shape((height, size), BF16), shape((size, height), BF16), shape((1, size), F32), row)
        raw, t, w, line, diagonal = call(
            functools.partial(prepare_body, parts), (shape((size, height), BF16), *made), [weight, diagonal, *pieces]
        )
        raw = lax.ppermute(raw, "col", sibling)
        turn, weigh, row, diagonal, strip = call(
            functools.partial(finish_body, parts),
            (*made, shape((width, 2 * size + sum(h.shape[1] for h in held)), BF16)),
            [weight, diagonal, raw, t, *held],
        )
        held[:] = [] if send else [strip]
        if send:
            routes = [from_owner[0], None if label in ("1", "2") else from_owner[1], from_owner[2]]
            above, far, below = (lax.ppermute(strip, ("col", "row"), perm) if perm else None for perm in routes)
            if far is None:
                far = lax.ppermute(below, ("col", "row"), onward)
            strips.extend([strip, above, far, below])
        rows.extend([line, row])
        turned.extend([t, turn])
        weighted.extend([w, weigh])

    def whole(*steps):
        return tuple((-2 * s, 0, own_pairs, 0) for s in steps)

    rest = 2 * own_pairs // 3
    group(whole(0, 1, -1, 2), [pair_density, rising[1], falling[1], rising[2]], False)
    group(whole(-2, 3, -3, 4), [falling[2], rising[3], falling[3], rising[4]], True)
    group(whole(-4, 5, -5, 6), [falling[4], rising[5], falling[5], rising[6]], True)
    group(whole(-6, 7) + ((14, 0, rest, 0),), [falling[6], rising[7], falling[7]], True)
    group(
        ((14, rest, own_pairs - rest, rest), (-16, 0, half, 0), (16, half, half, 0)),
        [falling[7], rising[8], falling[8]],
        True,
    )
    n, sent = len(weighted) // 2, len(strips) // 4

    size = pairs // count
    tall, flat = (width, size), (width, height)
    traded = shape((count, *tall), BF16)
    filled = pltpu.VMEM((width, pairs), BF16)
    operand = pltpu.VMEM(flat, BF16)

    def exchange(sends):
        parts = lax.all_to_all(sends, "row", split_axis=0, concat_axis=0, tiled=True)
        total = call(combine_body, shape(tall, BF16), [parts])
        around = [[(r, (r + shift) % count) for r in range(count)] for shift in SHIFTS]
        return [total, *(lax.ppermute(total, "row", perm) for perm in around)]

    epsilon, mixed, guess_rows, sends = call(
        functools.partial(start_body, n, sent),
        (shape(flat, F32), shape(flat, F32), shape((1, height), F32), traded),
        [sqrt_rows, sqrt_cols, scale_rows, scale_cols, diagonal, token, *strips, *rows, *weighted, *turned],
        [filled, operand, pltpu.VMEM((1, pairs), F32)],
        limit=12,
    )
    pieces = exchange(sends)
    square, sends = call(
        functools.partial(middle_body, 2 * n),
        (shape(flat, F32), traded),
        [sqrt_rows, guess_rows, mixed, *pieces, *weighted, *turned],
        [operand, filled],
        limit=12,
    )
    pieces = exchange(sends)
    inverse = call(
        functools.partial(final_body, 2 * n),
        shape(flat, F32),
        [sqrt_rows, guess_rows, mixed, square, *pieces, *weighted],
        [filled],
        limit=12,
    )
    return (epsilon.T, inverse.T)


def solution(mesh):
    placed = (P(("pb", "col"), "row"), P(), P(), P(), P(None, "pb"), P("pb"), P("pb"))

    return jax.shard_map(
        on_device,
        mesh=mesh,
        in_specs=placed,
        out_specs=(P(("pb", "row"), "col"), P(("pb", "row"), "col")),
        check_vma=False,
    )
```
